256 devices in a mesh: shots: 4 (over y, x), gx: 32 (over z), gy: 2 (over core).
Axes of the slice: x: 2, y: 2, z: 32, core: 2. Of those that a mesh axis runs over, the one named last changes fastest.
The devices are a block of a 4x8x32 slice.
Arguments:
- pressure: float32 [128, 1024, 256], P(None, ('shots', 'gx'), 'gy'), parts along dimension 1, may hold values from -6 to 6
- pressure_prior: float32 [128, 1024, 256], P(None, ('shots', 'gx'), 'gy'), parts along dimension 1, may hold values from -6 to 6
- courant_square: bfloat16 [128, 256, 256], P(None, 'gx', 'gy'), may hold values from 0.049804688 to 0.1796875
- wavelet: float32 [64], P('shots'), parts along dimension 0, may hold values from -4 to 4
- delay_steps: int32 [1024, 256], P(('shots', 'gx'), 'gy'), parts along dimension 0, may hold values from 0 to 7
- source_depth: int32 [1024, 256], P(('shots', 'gx'), 'gy'), parts along dimension 0, may hold values from 4 to 31
- receiver_depth: int32 [1024, 256], P(('shots', 'gx'), 'gy'), parts along dimension 0, may hold values from 0 to 31
- receiver_field: float32 [128, 1024, 256], P(None, ('shots', 'gx'), 'gy'), parts along dimension 1, may hold values from -6 to 6
Outputs:
- pressure_final: float32 [128, 1024, 256], P(None, ('shots', 'gx'), 'gy'), parts along dimension 1
- image: float32 [128, 1024, 256], P('gx', 'shots', 'gy'), parts along dimension 1
The draws below stay inside these ranges and needn't reach their ends.
There are 4 independent parts, one for each index of `shots`. The reference program is written for one: setup_inputs(seed, part) draws one part's arguments, and reference() takes and returns one part's arrays. A program takes and returns all parts, laid end to end along the dimension named above; an argument that names none is the same for every part. Nothing has to cross between parts.
All inputs are finite; a program needn't handle non-finite values.
Results may differ from the reference program's by a relative error of at most 0.00035.
Values sent between devices are 32-bit elements; how exact they have to be, the bound alone decides.
A program may use at most 64 MiB of HBM per device.

```python
import math
import jax
import jax.numpy as jnp

STEPS = 8
DMAX = 8
WAVE = 16
NX = 256
NY = 256
NZ = 128


def plant(array, stream_key, low, top_value):
    shape = array.shape
    spot = [jax.random.randint(jax.random.fold_in(stream_key, axis), (), 0, shape[axis]) for axis in range(len(shape))]
    array = array.at[tuple(spot)].set(low)
    longest = shape.index(max(shape))
    spot[longest] = (spot[longest] + 1) % shape[longest]
    return array.at[tuple(spot)].set(top_value)


def block_levels(rng, dims, cuts, low, high):
    def one(axis_at, parts):
        steps = jax.random.uniform(jax.random.fold_in(jax.random.fold_in(rng, 6), axis_at), (parts,), jnp.float32, low / len(cuts), high / len(cuts))
        return jnp.repeat(jnp.exp(steps), dims[axis_at] // parts).reshape((-1,) + (1,) * (len(dims) - axis_at - 1))

    factor_of = one(*cuts[0])
    for cut in cuts[1:]:
        factor_of = factor_of * one(*cut)
    return factor_of


def gaussian(key, dims, scale, most, split=(), kind=jnp.bfloat16):
    gain = block_levels(key, dims, split, -0.22, 0.18) if split else 1.0
    entries = jax.random.normal(key, dims, jnp.float32) * scale * gain
    return jnp.minimum(jnp.maximum(entries, -most), most).astype(kind)


def setup_inputs(seed: int = 0, part: int = 0) -> dict:
    seeds = jax.random.split(jax.random.key(seed), 9)
    own_keys = jax.random.split(jax.random.fold_in(seeds[8], part), 9)
    pressure = gaussian(own_keys[0], (NZ, NX, NY), 1.0, 6.0, ((1, 32), (2, 2)), jnp.float32)
    pressure_prior = gaussian(own_keys[1], (NZ, NX, NY), 1.0, 6.0, ((1, 32), (2, 2)), jnp.float32)
    courant_square = jnp.clip(jnp.exp(math.log(0.1796875) - 1.2831101 * jax.random.uniform(seeds[2], (NZ, NX, NY), jnp.float32) ** block_levels(seeds[2], (NZ, NX, NY), ((1, 32), (2, 2)), -0.2, 0.2)), 0.049804688, 0.1796875).astype(jnp.bfloat16)
    wavelet = gaussian(own_keys[3], (WAVE,), 1.0, 4.0, (), jnp.float32)
    delay_steps = plant(jax.random.randint(own_keys[4], (NX, NY), 0, DMAX), jax.random.fold_in(own_keys[4], 1), 0, DMAX - 1).astype(jnp.int32)
    source_depth = plant(jax.random.randint(own_keys[5], (NX, NY), 4, 32), jax.random.fold_in(own_keys[5], 1), 4, 31).astype(jnp.int32)
    receiver_depth = plant(jax.random.randint(own_keys[6], (NX, NY), 0, NZ // 4), jax.random.fold_in(own_keys[6], 1), 0, (NZ // 4) - 1).astype(jnp.int32)
    receiver_field = gaussian(own_keys[7], (NZ, NX, NY), 1.0, 6.0, ((1, 32), (2, 2)), jnp.float32)
    return dict(pressure=pressure, pressure_prior=pressure_prior, courant_square=courant_square, wavelet=wavelet, delay_steps=delay_steps, source_depth=source_depth, receiver_depth=receiver_depth, receiver_field=receiver_field)


CENTER = -205.0 / 72.0
COEFS = (1.6, -0.2, 8.0 / 315.0, -1.0 / 560.0)


def laplacian(field):
    depth, width, length = field.shape
    padded = jnp.pad(field, 4)
    total = (3.0 * CENTER) * field
    for k in range(1, 5):
        near = padded[4 + k:4 + k + depth, 4:4 + width, 4:4 + length] + padded[4 - k:4 - k + depth, 4:4 + width, 4:4 + length]
        near = near + padded[4:4 + depth, 4 + k:4 + k + width, 4:4 + length] + padded[4:4 + depth, 4 - k:4 - k + width, 4:4 + length]
        near = near + padded[4:4 + depth, 4:4 + width, 4 + k:4 + k + length] + padded[4:4 + depth, 4:4 + width, 4 - k:4 - k + length]
        total = total + COEFS[k - 1] * near
    return total


def injection(step, wavelet, delay_steps, source_depth, depth):
    picks = jnp.arange(wavelet.shape[0], dtype=jnp.int32)
    onehot = (picks[:, None, None] == (delay_steps + step)[None]).astype(wavelet.dtype)
    amplitude = jnp.sum(onehot * wavelet[:, None, None], axis=0)
    levels = jnp.arange(depth, dtype=jnp.int32)[:, None, None]
    return jnp.where(levels == source_depth[None], amplitude[None], jnp.zeros_like(amplitude)[None])


def reference(pressure, pressure_prior, courant_square, wavelet, delay_steps, source_depth, receiver_depth, receiver_field):
    depth = pressure.shape[0]
    coefficient = courant_square.astype(jnp.float32)
    current, prior = pressure, pressure_prior
    for step in range(STEPS):
        nxt = 2.0 * current - prior + coefficient * laplacian(current) + injection(step, wavelet, delay_steps, source_depth, depth)
        prior, current = current, nxt
    levels = jnp.arange(depth, dtype=jnp.int32)[:, None, None]
    masked = jnp.where(levels >= receiver_depth[None], receiver_field, jnp.zeros_like(receiver_field))
    product = current * masked
    padded = jnp.pad(product, ((1, 1), (0, 0), (0, 0)))
    image = 2.0 * product - padded[:-2] - padded[2:]
    return current, image
```

```python
import functools

import jax
import jax.numpy as jnp
from jax import lax
from jax.experimental import pallas as pl
from jax.experimental.pallas import tpu as pltpu
from jax.sharding import PartitionSpec as P

STEPS = 8
CENTER = -205.0 / 72.0
COEFS = (1.6, -0.2, 8.0 / 315.0, -1.0 / 560.0)
REACH = 4
ROWS = 16
PAIRS = ROWS // 2
MESH = pl.DeviceIdType.MESH


def kernel(
    ring,
    pressure, prior, courant, wavelet, delay, source, receiver, snapshot,
    final, image,
    field, courant_in, courant_f32, samples, delay_v, source_v, receiver_v, snapshot_v,
    amplitude, product, filtered,
    to_left, to_right, from_left, from_right, side,
    load_sem, left_send, right_send, side_send, left_recv, right_recv, side_recv,
    image_send, image_recv, out_sem, token_left, token_right,
):
    depth, width, lanes = pressure.shape
    chunks = depth // ROWS
    slab = depth // ring
    me, my_y = lax.axis_index("gx"), lax.axis_index("gy")
    right, left = lax.rem(me + 1, ring), lax.rem(me + ring - 1, ring)
    has_left, has_right = me > 0, me < ring - 1

    inner = pl.ds(REACH, depth)
    loads = [
        pltpu.make_async_copy(src, dst, load_sem.at[i])
        for i, (src, dst) in enumerate(
            (
                (pressure, field.at[0, inner]),
                (wavelet, samples),
                (delay, delay_v),
                (source, source_v),
                (prior, field.at[1, inner]),
                (courant, courant_in),
                (receiver, receiver_v),
                (snapshot, snapshot_v),
            )
        )
    ]
    for load in loads:
        load.start()

    barrier = pltpu.get_barrier_semaphore()
    for peer in ({"gx": left}, {"gx": right}, {"gy": 1 - my_y}):
        pl.semaphore_signal(barrier, inc=1, device_id=peer, device_id_type=MESH)

    zero = jnp.zeros((width, lanes), jnp.float32)
    for half in range(2):
        for i in range(REACH):
            field[half, i] = zero
            field[half, depth + REACH + i] = zero
    product[0] = zero
    product[depth + 1] = zero

    @pl.when(jnp.logical_not(has_left))
    def _():
        from_left[...] = jnp.zeros_like(from_left)

    @pl.when(jnp.logical_not(has_right))
    def _():
        from_right[...] = jnp.zeros_like(from_right)

    sub = lax.broadcasted_iota(jnp.int32, (width, lanes), 0)
    lane = lax.broadcasted_iota(jnp.int32, (width, lanes), 1)
    low = sub < REACH
    facing = (lane // (lanes // 2)) == my_y

    def left_copy(slot, c):
        return pltpu.make_async_remote_copy(
            to_left.at[slot, c], from_right.at[slot, c], left_send.at[slot, c],
            right_recv.at[slot, c], device_id={"gx": left}, device_id_type=MESH,
        )

    def right_copy(slot, c):
        return pltpu.make_async_remote_copy(
            to_right.at[slot, c], from_left.at[slot, c], right_send.at[slot, c],
            left_recv.at[slot, c], device_id={"gx": right}, device_id_type=MESH,
        )

    def side_copy(slot, c):
        return pltpu.make_async_remote_copy(
            field.at[slot, pl.ds(REACH + c * ROWS, ROWS)], side.at[slot, pl.ds(c * ROWS, ROWS)],
            side_send.at[slot, c], side_recv.at[slot, c],
            device_id={"gy": 1 - my_y}, device_id_type=MESH,
        )

    def send(slot, c):
        @pl.when(has_left)
        def _():
            left_copy(slot, c).start()

        @pl.when(has_right)
        def _():
            right_copy(slot, c).start()

        side_copy(slot, c).start()

    def sent(slot, c):
        @pl.when(has_left)
        def _():
            left_copy(slot, c).wait_send()

        @pl.when(has_right)
        def _():
            right_copy(slot, c).wait_send()

        side_copy(slot, c).wait_send()

    def arrived(slot, c):
        @pl.when(has_left)
        def _():
            right_copy(slot, c).wait_recv()

        @pl.when(has_right)
        def _():
            left_copy(slot, c).wait_recv()

        side_copy(slot, c).wait_recv()

    def pack(slot, c, i, first, second):
        turned = pltpu.roll(second, REACH, 0)
        to_left[slot, c, i] = jnp.where(low, first, turned)
        to_right[slot, c, i] = jnp.where(low, turned, first)

    def rounds(c):
        @pl.when(lax.rem(c, 4) == 0)
        def _():
            pl.semaphore_signal(token_right, inc=1, device_id={"gx": left}, device_id_type=MESH)
            pl.semaphore_signal(token_left, inc=1, device_id={"gx": right}, device_id_type=MESH)

        @pl.when(lax.rem(c, 4) == 3)
        def _():
            pl.semaphore_wait(token_left, 1)
            pl.semaphore_wait(token_right, 1)

    def advanced(now, later, c, z, halo, amp, where_from):
        at = z + REACH
        mine = field[now, at]
        beside = jnp.where(facing, side[now, z], 0.0)
        total = (3.0 * CENTER) * mine
        for k in range(1, REACH + 1):
            near = field[now, at + k] + field[now, at - k]
            if k == REACH:
                near = near + pltpu.roll(mine + halo, k, 0)
            else:
                near = near + pltpu.roll(jnp.where(sub >= k, mine, halo), width - k, 0)
                near = near + pltpu.roll(jnp.where(sub < width - k, mine, halo), k, 0)
            near = near + pltpu.roll(jnp.where(lane >= k, mine, beside), lanes - k, 1)
            near = near + pltpu.roll(jnp.where(lane < lanes - k, mine, beside), k, 1)
            total = total + COEFS[k - 1] * near
        added = jnp.where(where_from == z, amp, 0.0)
        return 2.0 * mine - field[later, at] + courant_f32[z] * total + added

    def halos(now, c, i):
        a, b = from_left[now, c, i], from_right[now, c, i]
        return jnp.where(low, b, a), pltpu.roll(jnp.where(low, a, b), REACH, 0)

    loads[0].wait()
    pl.semaphore_wait(barrier, 3)

    def open_chunk(c, _):
        for i in range(PAIRS):
            z = c * ROWS + 2 * i + REACH
            pack(0, c, i, field[0, z], field[0, z + 1])
        send(0, c)
        return 0

    lax.fori_loop(0, chunks, open_chunk, 0)

    for load in loads[1:]:
        load.wait()
    when = delay_v[...]
    for t in range(STEPS):
        amp = jnp.zeros((width, lanes), jnp.float32)
        for pick in range(samples.shape[0]):
            amp = amp + jnp.where(when + t == pick, samples[pick], 0.0)
        amplitude[t] = amp

    def widen(c, _):
        for i in range(ROWS):
            courant_f32[c * ROWS + i] = courant_in[c * ROWS + i].astype(jnp.float32)
        return 0

    lax.fori_loop(0, chunks, widen, 0)

    def step(t, _):
        now, later = lax.rem(t, 2), lax.rem(t + 1, 2)

        def chunk(c, _):
            rounds(c)
            arrived(now, c)

            @pl.when(t > 0)
            def _():
                sent(later, c)

            amp, where_from = amplitude[t], source_v[...]
            for i in range(PAIRS):
                z = c * ROWS + 2 * i
                new = [
                    advanced(now, later, c, z + j, halo, amp, where_from)
                    for j, halo in enumerate(halos(now, c, i))
                ]
                field[later, z + REACH] = new[0]
                field[later, z + REACH + 1] = new[1]
                pack(later, c, i, *new)
            send(later, c)
            return 0

        lax.fori_loop(0, chunks, chunk, 0)
        return 0

    lax.fori_loop(0, STEPS - 1, step, 0)

    now, later = (STEPS - 1) % 2, STEPS % 2

    def last_chunk(c, _):
        rounds(c)
        arrived(now, c)
        sent(later, c)
        amp, where_from, first_level = amplitude[STEPS - 1], source_v[...], receiver_v[...]
        for i in range(PAIRS):
            for j, halo in enumerate(halos(now, c, i)):
                z = c * ROWS + 2 * i + j
                new = advanced(now, later, c, z, halo, amp, where_from)
                field[later, z + REACH] = new
                product[z + 1] = new * jnp.where(first_level <= z, snapshot_v[z], 0.0)
        return 0

    lax.fori_loop(0, chunks, last_chunk, 0)

    keep = pltpu.make_async_copy(field.at[later, inner], final, out_sem.at[0])

    def image_chunk(c, _):
        for i in range(ROWS):
            z = c * ROWS + i
            filtered[z] = 2.0 * product[z + 1] - product[z] - product[z + 2]
        return 0

    lax.fori_loop(0, chunks, image_chunk, 0)

    def block(owner):
        return filtered.at[pl.ds(owner * slab, slab)]

    def place(owner):
        return image.at[:, pl.ds(pl.multiple_of(owner * width, width), width), :]

    def image_copy(owner):
        return pltpu.make_async_remote_copy(
            block(owner), place(me), image_send.at[owner], image_recv.at[me],
            device_id={"gx": owner}, device_id_type=MESH,
        )

    def image_in(origin):
        return pltpu.make_async_remote_copy(
            block(origin), place(origin), image_send.at[origin], image_recv.at[origin],
            device_id={"gx": origin}, device_id_type=MESH,
        )

    half = ring // 2
    image_copy(lax.rem(me + half, ring)).start()

    def spread(i, _):
        k = half - 1 - i
        image_copy(lax.rem(me + k, ring)).start()
        image_copy(lax.rem(me + ring - k, ring)).start()
        return 0

    lax.fori_loop(0, half - 1, spread, 0)
    own = pltpu.make_async_copy(block(me), place(me), out_sem.at[1])
    own.start()
    keep.start()

    def drain(c, _):
        sent(now, c)
        return 0

    lax.fori_loop(0, chunks, drain, 0)
    own.wait()
    keep.wait()

    def collect(i, _):
        other = lax.rem(me + 1 + i, ring)
        image_in(other).wait_recv()
        image_copy(other).wait_send()
        return 0

    lax.fori_loop(0, ring - 1, collect, 0)


def shards(ring, *args):
    pressure = args[0]
    depth, width, lanes = pressure.shape
    chunks, slab = depth // ROWS, depth // ring
    tile = (width, lanes)
    f32 = jnp.float32
    packets = pltpu.VMEM((2, chunks, PAIRS) + tile, f32)
    dma = pltpu.SemaphoreType.DMA
    return pl.pallas_call(
        functools.partial(kernel, ring),
        out_shape=(
            jax.ShapeDtypeStruct((depth,) + tile, f32),
            jax.ShapeDtypeStruct((slab, ring * width, lanes), f32),
        ),
        in_specs=[pl.BlockSpec(memory_space=pl.ANY)] * 8,
        out_specs=[pl.BlockSpec(memory_space=pl.ANY)] * 2,
        scratch_shapes=[
            pltpu.VMEM((2, depth + 2 * REACH) + tile, f32),
            pltpu.VMEM((depth,) + tile, jnp.bfloat16),
            pltpu.VMEM((depth,) + tile, f32),
            pltpu.SMEM(args[3].shape, f32),
            pltpu.VMEM(tile, jnp.int32),
            pltpu.VMEM(tile, jnp.int32),
            pltpu.VMEM(tile, jnp.int32),
            pltpu.VMEM((depth,) + tile, f32),
            pltpu.VMEM((STEPS,) + tile, f32),
            pltpu.VMEM((depth + 2,) + tile, f32),
            pltpu.VMEM((depth,) + tile, f32),
            packets, packets, packets, packets,
            pltpu.VMEM((2, depth) + tile, f32),
            dma((8,)),
            dma((2, chunks)), dma((2, chunks)), dma((2, chunks)),
            dma((2, chunks)), dma((2, chunks)), dma((2, chunks)),
            dma((ring,)), dma((ring,)), dma((2,)),
            pltpu.SemaphoreType.REGULAR, pltpu.SemaphoreType.REGULAR,
        ],
        compiler_params=pltpu.CompilerParams(collective_id=0, has_side_effects=True),
        name="march",
    )(*args)


def solution(mesh):
    in_specs = (
        P(None, ("shots", "gx"), "gy"),
        P(None, ("shots", "gx"), "gy"),
        P(None, "gx", "gy"),
        P("shots"),
        P(("shots", "gx"), "gy"),
        P(("shots", "gx"), "gy"),
        P(("shots", "gx"), "gy"),
        P(None, ("shots", "gx"), "gy"),
    )
    out_specs = (P(None, ("shots", "gx"), "gy"), P("gx", "shots", "gy"))
    return jax.shard_map(
        functools.partial(shards, mesh.shape["gx"]),
        mesh=mesh, in_specs=in_specs, out_specs=out_specs, check_vma=False,
    )
```

```python
import functools

import jax
import jax.numpy as jnp
from jax import lax
from jax.experimental import pallas as pl
from jax.experimental.pallas import tpu as pltpu
from jax.sharding import PartitionSpec as P

STEPS = 8
CENTER = -205.0 / 72.0
COEFS = (1.6, -0.2, 8.0 / 315.0, -1.0 / 560.0)
REACH = 4
ROWS = 32
PAIRS = ROWS // 2
MESH = pl.DeviceIdType.MESH


def kernel(
    ring,
    pressure, prior, courant, wavelet, delay, source, receiver, snapshot,
    final, image,
    field, courant_in, courant_f32, samples, delay_v, source_v, receiver_v, snapshot_v,
    amplitude, product, filtered,
    to_left, to_right, from_left, from_right, side,
    chunk_sem, load_sem, left_send, right_send, side_send, left_recv, right_recv, side_recv,
    image_send, image_recv, out_sem, token_left, token_right,
):
    depth, width, lanes = pressure.shape
    chunks = depth // ROWS
    slab = depth // ring
    me, my_y = lax.axis_index("gx"), lax.axis_index("gy")
    right, left = lax.rem(me + 1, ring), lax.rem(me + ring - 1, ring)
    has_left, has_right = me > 0, me < ring - 1

    barrier = pltpu.get_barrier_semaphore()
    for peer in ({"gx": left}, {"gx": right}, {"gy": 1 - my_y}):
        pl.semaphore_signal(barrier, inc=1, device_id=peer, device_id_type=MESH)

    def load_chunk(c):
        return pltpu.make_async_copy(
            pressure.at[pl.ds(c * ROWS, ROWS)], field.at[0, pl.ds(REACH + c * ROWS, ROWS)],
            chunk_sem.at[c],
        )

    for c in range(chunks):
        load_chunk(c).start()
    inner = pl.ds(REACH, depth)
    loads = [
        pltpu.make_async_copy(src, dst, load_sem.at[i])
        for i, (src, dst) in enumerate(
            (
                (wavelet, samples),
                (delay, delay_v),
                (source, source_v),
                (prior, field.at[1, inner]),
                (courant, courant_in),
                (receiver, receiver_v),
                (snapshot, snapshot_v),
            )
        )
    ]
    for load in loads:
        load.start()

    zero = jnp.zeros((width, lanes), jnp.float32)
    for half in range(2):
        for i in range(REACH):
            field[half, i] = zero
            field[half, depth + REACH + i] = zero
    product[0] = zero
    product[depth + 1] = zero

    @pl.when(jnp.logical_not(has_left))
    def _():
        from_left[...] = jnp.zeros_like(from_left)

    @pl.when(jnp.logical_not(has_right))
    def _():
        from_right[...] = jnp.zeros_like(from_right)

    sub = lax.broadcasted_iota(jnp.int32, (width, lanes), 0)
    lane = lax.broadcasted_iota(jnp.int32, (width, lanes), 1)
    low = sub < REACH
    facing = (lane // (lanes // 2)) == my_y

    def left_copy(slot, c):
        return pltpu.make_async_remote_copy(
            to_left.at[slot, c], from_right.at[slot, c], left_send.at[slot, c],
            right_recv.at[slot, c], device_id={"gx": left}, device_id_type=MESH,
        )

    def right_copy(slot, c):
        return pltpu.make_async_remote_copy(
            to_right.at[slot, c], from_left.at[slot, c], right_send.at[slot, c],
            left_recv.at[slot, c], device_id={"gx": right}, device_id_type=MESH,
        )

    def side_copy(slot, c):
        return pltpu.make_async_remote_copy(
            field.at[slot, pl.ds(REACH + c * ROWS, ROWS)], side.at[slot, pl.ds(c * ROWS, ROWS)],
            side_send.at[slot, c], side_recv.at[slot, c],
            device_id={"gy": 1 - my_y}, device_id_type=MESH,
        )

    def send(slot, c):
        @pl.when(has_left)
        def _():
            left_copy(slot, c).start()

        @pl.when(has_right)
        def _():
            right_copy(slot, c).start()

        side_copy(slot, c).start()

    def sent(slot, c):
        @pl.when(has_left)
        def _():
            left_copy(slot, c).wait_send()

        @pl.when(has_right)
        def _():
            right_copy(slot, c).wait_send()

        side_copy(slot, c).wait_send()

    def arrived(slot, c):
        @pl.when(has_left)
        def _():
            right_copy(slot, c).wait_recv()

        @pl.when(has_right)
        def _():
            left_copy(slot, c).wait_recv()

        side_copy(slot, c).wait_recv()

    def pack(slot, c, i, first, second):
        turned = pltpu.roll(second, REACH, 0)
        to_left[slot, c, i] = jnp.where(low, first, turned)
        to_right[slot, c, i] = jnp.where(low, turned, first)

    def rounds(c):
        @pl.when(lax.rem(c, 2) == 0)
        def _():
            pl.semaphore_signal(token_right, inc=1, device_id={"gx": left}, device_id_type=MESH)
            pl.semaphore_signal(token_left, inc=1, device_id={"gx": right}, device_id_type=MESH)

        @pl.when(lax.rem(c, 2) == 1)
        def _():
            pl.semaphore_wait(token_left, 1)
            pl.semaphore_wait(token_right, 1)

    def advanced(now, later, c, z, halo, amp, where_from):
        at = z + REACH
        mine = field[now, at]
        beside = jnp.where(facing, side[now, z], 0.0)
        total = (3.0 * CENTER) * mine
        for k in range(1, REACH + 1):
            near = field[now, at + k] + field[now, at - k]
            if k == REACH:
                near = near + pltpu.roll(mine + halo, k, 0)
            else:
                near = near + pltpu.roll(jnp.where(sub >= k, mine, halo), width - k, 0)
                near = near + pltpu.roll(jnp.where(sub < width - k, mine, halo), k, 0)
            near = near + pltpu.roll(jnp.where(lane >= k, mine, beside), lanes - k, 1)
            near = near + pltpu.roll(jnp.where(lane < lanes - k, mine, beside), k, 1)
            total = total + COEFS[k - 1] * near
        added = jnp.where(where_from == z, amp, 0.0)
        return 2.0 * mine - field[later, at] + courant_f32[z] * total + added

    def halos(now, c, i):
        a, b = from_left[now, c, i], from_right[now, c, i]
        return jnp.where(low, b, a), pltpu.roll(jnp.where(low, a, b), REACH, 0)

    pl.semaphore_wait(barrier, 3)

    def open_chunk(c, _):
        load_chunk(c).wait()
        for i in range(PAIRS):
            z = c * ROWS + 2 * i + REACH
            pack(0, c, i, field[0, z], field[0, z + 1])
        send(0, c)
        return 0

    lax.fori_loop(0, chunks, open_chunk, 0)

    for load in loads:
        load.wait()
    when = delay_v[...]
    for t in range(STEPS):
        amp = jnp.zeros((width, lanes), jnp.float32)
        for pick in range(samples.shape[0]):
            amp = amp + jnp.where(when + t == pick, samples[pick], 0.0)
        amplitude[t] = amp

    def widen(c, _):
        for i in range(ROWS):
            courant_f32[c * ROWS + i] = courant_in[c * ROWS + i].astype(jnp.float32)
        return 0

    lax.fori_loop(0, chunks, widen, 0)

    def step(t, _):
        now, later = lax.rem(t, 2), lax.rem(t + 1, 2)

        def chunk(c, _):
            rounds(c)
            arrived(now, c)

            @pl.when(t > 0)
            def _():
                sent(later, c)

            amp, where_from = amplitude[t], source_v[...]
            for i in range(PAIRS):
                z = c * ROWS + 2 * i
                new = [
                    advanced(now, later, c, z + j, halo, amp, where_from)
                    for j, halo in enumerate(halos(now, c, i))
                ]
                field[later, z + REACH] = new[0]
                field[later, z + REACH + 1] = new[1]
                pack(later, c, i, *new)
            send(later, c)
            return 0

        lax.fori_loop(0, chunks, chunk, 0)
        return 0

    lax.fori_loop(0, STEPS - 1, step, 0)

    now, later = (STEPS - 1) % 2, STEPS % 2

    def last_chunk(c, _):
        rounds(c)
        arrived(now, c)
        sent(later, c)
        amp, where_from, first_level = amplitude[STEPS - 1], source_v[...], receiver_v[...]
        for i in range(PAIRS):
            for j, halo in enumerate(halos(now, c, i)):
                z = c * ROWS + 2 * i + j
                new = advanced(now, later, c, z, halo, amp, where_from)
                final[z] = new
                product[z + 1] = new * jnp.where(first_level <= z, snapshot_v[z], 0.0)
        return 0

    lax.fori_loop(0, chunks, last_chunk, 0)

    def image_chunk(c, _):
        for i in range(ROWS):
            z = c * ROWS + i
            filtered[z] = 2.0 * product[z + 1] - product[z] - product[z + 2]
        return 0

    lax.fori_loop(0, chunks, image_chunk, 0)

    def block(owner):
        return filtered.at[pl.ds(owner * slab, slab)]

    def place(owner):
        return image.at[:, pl.ds(pl.multiple_of(owner * width, width), width), :]

    def image_copy(owner):
        return pltpu.make_async_remote_copy(
            block(owner), place(me), image_send, image_recv,
            device_id={"gx": owner}, device_id_type=MESH,
        )

    half = ring // 2
    image_copy(lax.rem(me + half, ring)).start()

    def spread(i, _):
        k = half - 1 - i
        image_copy(lax.rem(me + k, ring)).start()
        image_copy(lax.rem(me + ring - k, ring)).start()
        return 0

    lax.fori_loop(0, half - 1, spread, 0)
    own = pltpu.make_async_copy(block(me), place(me), out_sem)
    own.start()

    def drain(c, _):
        sent(now, c)
        return 0

    lax.fori_loop(0, chunks, drain, 0)
    own.wait()

    rest = image.at[:, pl.ds(0, (ring - 1) * width), :]
    pltpu.make_async_copy(rest, rest, image_recv).wait()
    pltpu.make_async_copy(rest, rest, image_send).wait()


def put(final_in, image_in, final, image, sems):
    copies = [
        pltpu.make_async_copy(final_in, final, sems.at[0]),
        pltpu.make_async_copy(image_in, image, sems.at[1]),
    ]
    for copy in copies:
        copy.start()
    for copy in copies:
        copy.wait()


def shards(ring, *args):
    pressure = args[0]
    depth, width, lanes = pressure.shape
    chunks, slab = depth // ROWS, depth // ring
    tile = (width, lanes)
    f32 = jnp.float32
    packets = pltpu.VMEM((2, chunks, PAIRS) + tile, f32)
    dma = pltpu.SemaphoreType.DMA
    shapes = ((depth,) + tile, (slab, ring * width, lanes))
    held = pl.pallas_call(
        functools.partial(kernel, ring),
        out_shape=tuple(pltpu.VMEM(shape, f32) for shape in shapes),
        in_specs=[pl.BlockSpec(memory_space=pl.ANY)] * 8,
        out_specs=[pl.BlockSpec(memory_space=pltpu.VMEM)] * 2,
        scratch_shapes=[
            pltpu.VMEM((2, depth + 2 * REACH) + tile, f32),
            pltpu.VMEM((depth,) + tile, jnp.bfloat16),
            pltpu.VMEM((depth,) + tile, f32),
            pltpu.SMEM(args[3].shape, f32),
            pltpu.VMEM(tile, jnp.int32),
            pltpu.VMEM(tile, jnp.int32),
            pltpu.VMEM(tile, jnp.int32),
            pltpu.VMEM((depth,) + tile, f32),
            pltpu.VMEM((STEPS,) + tile, f32),
            pltpu.VMEM((depth + 2,) + tile, f32),
            pltpu.VMEM((depth,) + tile, f32),
            packets, packets, packets, packets,
            pltpu.VMEM((2, depth) + tile, f32),
            dma((chunks,)), dma((7,)),
            dma((2, chunks)), dma((2, chunks)), dma((2, chunks)),
            dma((2, chunks)), dma((2, chunks)), dma((2, chunks)),
            dma, dma, dma,
            pltpu.SemaphoreType.REGULAR, pltpu.SemaphoreType.REGULAR,
        ],
        compiler_params=pltpu.CompilerParams(collective_id=0, has_side_effects=True),
        name="march",
    )(*args)
    return pl.pallas_call(
        put,
        out_shape=tuple(jax.ShapeDtypeStruct(shape, f32) for shape in shapes),
        in_specs=[pl.BlockSpec(memory_space=pltpu.VMEM)] * 2,
        out_specs=[pl.BlockSpec(memory_space=pl.ANY)] * 2,
        scratch_shapes=[dma((2,))],
        name="put",
    )(*(pltpu.with_memory_space_constraint(x, pltpu.VMEM) for x in held))


def solution(mesh):
    in_specs = (
        P(None, ("shots", "gx"), "gy"),
        P(None, ("shots", "gx"), "gy"),
        P(None, "gx", "gy"),
        P("shots"),
        P(("shots", "gx"), "gy"),
        P(("shots", "gx"), "gy"),
        P(("shots", "gx"), "gy"),
        P(None, ("shots", "gx"), "gy"),
    )
    out_specs = (P(None, ("shots", "gx"), "gy"), P("gx", "shots", "gy"))
    return jax.shard_map(
        functools.partial(shards, mesh.shape["gx"]),
        mesh=mesh, in_specs=in_specs, out_specs=out_specs, check_vma=False,
    )
```

```python
import functools

import jax
import jax.numpy as jnp
from jax import lax
from jax.experimental import pallas as pl
from jax.experimental.pallas import tpu as pltpu
from jax.sharding import PartitionSpec as P

STEPS = 8
CENTER = -205.0 / 72.0
COEFS = (1.6, -0.2, 8.0 / 315.0, -1.0 / 560.0)
REACH = 4
ROWS = 32
PAIRS = ROWS // 2
GROUP = 4
EARLY = 10
MESH = pl.DeviceIdType.MESH


def kernel(
    ring,
    pressure, prior, courant, wavelet, delay, source, receiver, snapshot,
    final, image,
    field, courant_in, courant_f32, samples, delay_v, source_v, receiver_v, snapshot_v,
    amplitude, product, filtered,
    to_left, to_right, from_left, from_right, side,
    chunk_sem, load_sem, left_send, right_send, side_send, left_recv, right_recv, side_recv,
    image_send, image_recv, out_sem, token_left, token_right,
):
    depth, width, lanes = pressure.shape
    chunks = depth // ROWS
    slab = depth // ring
    me, my_y = lax.axis_index("gx"), lax.axis_index("gy")
    right, left = lax.rem(me + 1, ring), lax.rem(me + ring - 1, ring)
    has_left, has_right = me > 0, me < ring - 1

    barrier = pltpu.get_barrier_semaphore()
    for peer in ({"gx": left}, {"gx": right}, {"gy": 1 - my_y}):
        pl.semaphore_signal(barrier, inc=1, device_id=peer, device_id_type=MESH)

    def load_chunk(c):
        return pltpu.make_async_copy(
            pressure.at[pl.ds(c * ROWS, ROWS)], field.at[0, pl.ds(REACH + c * ROWS, ROWS)],
            chunk_sem.at[c],
        )

    for c in range(chunks):
        load_chunk(c).start()
    inner = pl.ds(REACH, depth)
    loads = [
        pltpu.make_async_copy(src, dst, load_sem.at[i])
        for i, (src, dst) in enumerate(
            (
                (wavelet, samples),
                (delay, delay_v),
                (source, source_v),
                (prior, field.at[1, inner]),
                (courant, courant_in),
                (receiver, receiver_v),
                (snapshot, snapshot_v),
            )
        )
    ]
    for load in loads:
        load.start()

    zero = jnp.zeros((width, lanes), jnp.float32)
    for half in range(2):
        for i in range(REACH):
            field[half, i] = zero
            field[half, depth + REACH + i] = zero
    for i in range(slab + 1):
        product[i] = zero
    product[slab + depth + 1] = zero

    @pl.when(jnp.logical_not(has_left))
    def _():
        from_left[...] = jnp.zeros_like(from_left)

    @pl.when(jnp.logical_not(has_right))
    def _():
        from_right[...] = jnp.zeros_like(from_right)

    sub = lax.broadcasted_iota(jnp.int32, (width, lanes), 0)
    lane = lax.broadcasted_iota(jnp.int32, (width, lanes), 1)
    low = sub < REACH
    facing = (lane // (lanes // 2)) == my_y

    def left_copy(slot, c):
        return pltpu.make_async_remote_copy(
            to_left.at[slot, c], from_right.at[slot, c], left_send.at[slot, c],
            right_recv.at[slot, c], device_id={"gx": left}, device_id_type=MESH,
        )

    def right_copy(slot, c):
        return pltpu.make_async_remote_copy(
            to_right.at[slot, c], from_left.at[slot, c], right_send.at[slot, c],
            left_recv.at[slot, c], device_id={"gx": right}, device_id_type=MESH,
        )

    def side_copy(slot, c):
        return pltpu.make_async_remote_copy(
            field.at[slot, pl.ds(REACH + c * ROWS, ROWS)], side.at[slot, pl.ds(c * ROWS, ROWS)],
            side_send.at[slot, c], side_recv.at[slot, c],
            device_id={"gy": 1 - my_y}, device_id_type=MESH,
        )

    def send(slot, c):
        @pl.when(has_left)
        def _():
            left_copy(slot, c).start()

        @pl.when(has_right)
        def _():
            right_copy(slot, c).start()

        side_copy(slot, c).start()

    def sent(slot, c):
        @pl.when(has_left)
        def _():
            left_copy(slot, c).wait_send()

        @pl.when(has_right)
        def _():
            right_copy(slot, c).wait_send()

        side_copy(slot, c).wait_send()

    def arrived(slot, c):
        @pl.when(has_left)
        def _():
            right_copy(slot, c).wait_recv()

        @pl.when(has_right)
        def _():
            left_copy(slot, c).wait_recv()

        side_copy(slot, c).wait_recv()

    def pack(slot, c, i, first, second):
        turned = pltpu.roll(second, REACH, 0)
        to_left[slot, c, i] = jnp.where(low, first, turned)
        to_right[slot, c, i] = jnp.where(low, turned, first)

    def tell():
        pl.semaphore_signal(token_right, inc=1, device_id={"gx": left}, device_id_type=MESH)
        pl.semaphore_signal(token_left, inc=1, device_id={"gx": right}, device_id_type=MESH)

    def hear():
        pl.semaphore_wait(token_left, 1)
        pl.semaphore_wait(token_right, 1)

    def rounds(c):
        pl.when(lax.rem(c, 2) == 0)(tell)
        pl.when(lax.rem(c, 2) == 1)(hear)

    def advanced(now, later, z, halo, amp, where_from):
        at = z + REACH
        mine = field[now, at]
        beside = jnp.where(facing, side[now, z], 0.0)
        total = (3.0 * CENTER) * mine
        for k in range(1, REACH + 1):
            near = field[now, at + k] + field[now, at - k]
            if k == REACH:
                near = near + pltpu.roll(mine + halo, k, 0)
            else:
                near = near + pltpu.roll(jnp.where(sub >= k, mine, halo), width - k, 0)
                near = near + pltpu.roll(jnp.where(sub < width - k, mine, halo), k, 0)
            near = near + pltpu.roll(jnp.where(lane >= k, mine, beside), lanes - k, 1)
            near = near + pltpu.roll(jnp.where(lane < lanes - k, mine, beside), k, 1)
            total = total + COEFS[k - 1] * near
        added = jnp.where(where_from == z, amp, 0.0)
        return 2.0 * mine - field[later, at] + courant_f32[z] * total + added

    def halos(now, c, i):
        a, b = from_left[now, c, i], from_right[now, c, i]
        return jnp.where(low, b, a), pltpu.roll(jnp.where(low, a, b), REACH, 0)

    pl.semaphore_wait(barrier, 3)
    tell()

    def open_chunk(c, _):
        load_chunk(c).wait()
        for i in range(PAIRS):
            z = c * ROWS + 2 * i + REACH
            pack(0, c, i, field[0, z], field[0, z + 1])
        send(0, c)
        return 0

    lax.fori_loop(0, chunks, open_chunk, 0)

    for load in loads:
        load.wait()
    when = delay_v[...]
    for t in range(STEPS):
        amp = jnp.zeros((width, lanes), jnp.float32)
        for pick in range(samples.shape[0]):
            amp = amp + jnp.where(when + t == pick, samples[pick], 0.0)
        amplitude[t] = amp

    def widen(c, _):
        for i in range(ROWS):
            courant_f32[c * ROWS + i] = courant_in[c * ROWS + i].astype(jnp.float32)
        return 0

    lax.fori_loop(0, chunks, widen, 0)
    hear()

    def step(t, _):
        now, later = lax.rem(t, 2), lax.rem(t + 1, 2)

        def chunk(c, _):
            rounds(c)
            arrived(now, c)

            @pl.when(t > 0)
            def _():
                sent(later, c)

            amp, where_from = amplitude[t], source_v[...]
            for first in range(0, PAIRS, GROUP):
                pairs = [
                    [
                        advanced(now, later, c * ROWS + 2 * i + j, halo, amp, where_from)
                        for j, halo in enumerate(halos(now, c, i))
                    ]
                    for i in range(first, first + GROUP)
                ]
                for i, new in enumerate(pairs, first):
                    z = c * ROWS + 2 * i
                    field[later, z + REACH] = new[0]
                    field[later, z + REACH + 1] = new[1]
                    pack(later, c, i, *new)
            send(later, c)
            return 0

        lax.fori_loop(0, chunks, chunk, 0)
        return 0

    lax.fori_loop(0, STEPS - 1, step, 0)

    now, later = (STEPS - 1) % 2, STEPS % 2

    def block(owner):
        return filtered.at[pl.ds(slab + owner * slab, slab)]

    def place(owner):
        return image.at[:, pl.ds(pl.multiple_of(owner * width, width), width), :]

    def image_copy(owner):
        return pltpu.make_async_remote_copy(
            block(owner), place(me), image_send, image_recv,
            device_id={"gx": owner}, device_id_type=MESH,
        )

    half, owners = ring // 2, ROWS // slab

    def filter_row(first, count):
        for i in range(count):
            z = slab + first + i
            filtered[z] = 2.0 * product[z + 1] - product[z] - product[z + 2]

    def early(owner):
        ahead = lax.rem(owner - me + ring, ring)
        far = jnp.minimum(ahead, ring - ahead) >= EARLY
        return far & (owner >= 0) & (owner < (chunks - 1) * owners - 1)

    def last_chunk(c, _):
        arrived(now, c)
        sent(later, c)
        amp, where_from, first_level = amplitude[STEPS - 1], source_v[...], receiver_v[...]
        for i in range(PAIRS):
            for j, halo in enumerate(halos(now, c, i)):
                z = c * ROWS + 2 * i + j
                new = advanced(now, later, z, halo, amp, where_from)
                final[z] = new
                product[slab + z + 1] = new * jnp.where(first_level <= z, snapshot_v[z], 0.0)
        filter_row(c * ROWS - slab, ROWS)
        for i in range(owners):
            owner = c * owners - 1 + i

            @pl.when(early(owner))
            def _():
                image_copy(owner).start()

        return 0

    lax.fori_loop(0, chunks, last_chunk, 0)

    filter_row(depth - slab, slab)

    def send_block(owner):
        @pl.when(jnp.logical_not(early(owner)))
        def _():
            image_copy(owner).start()

    send_block(lax.rem(me + half, ring))

    def spread(i, _):
        k = half - 1 - i
        send_block(lax.rem(me + k, ring))
        send_block(lax.rem(me + ring - k, ring))
        return 0

    lax.fori_loop(0, half - 1, spread, 0)
    own = pltpu.make_async_copy(block(me), place(me), out_sem)
    own.start()

    def drain(c, _):
        sent(now, c)
        return 0

    lax.fori_loop(0, chunks, drain, 0)
    own.wait()

    rest = image.at[:, pl.ds(0, (ring - 1) * width), :]
    pltpu.make_async_copy(rest, rest, image_recv).wait()
    pltpu.make_async_copy(rest, rest, image_send).wait()


def put(final_in, image_in, final, image, sems):
    copies = [
        pltpu.make_async_copy(final_in, final, sems.at[0]),
        pltpu.make_async_copy(image_in, image, sems.at[1]),
    ]
    for copy in copies:
        copy.start()
    for copy in copies:
        copy.wait()


def shards(ring, *args):
    pressure = args[0]
    depth, width, lanes = pressure.shape
    chunks, slab = depth // ROWS, depth // ring
    tile = (width, lanes)
    f32 = jnp.float32
    packets = pltpu.VMEM((2, chunks, PAIRS) + tile, f32)
    dma = pltpu.SemaphoreType.DMA
    shapes = ((depth,) + tile, (slab, ring * width, lanes))
    held = pl.pallas_call(
        functools.partial(kernel, ring),
        out_shape=tuple(pltpu.VMEM(shape, f32) for shape in shapes),
        in_specs=[pl.BlockSpec(memory_space=pl.ANY)] * 8,
        out_specs=[pl.BlockSpec(memory_space=pltpu.VMEM)] * 2,
        scratch_shapes=[
            pltpu.VMEM((2, depth + 2 * REACH) + tile, f32),
            pltpu.VMEM((depth,) + tile, jnp.bfloat16),
            pltpu.VMEM((depth,) + tile, f32),
            pltpu.SMEM(args[3].shape, f32),
            pltpu.VMEM(tile, jnp.int32),
            pltpu.VMEM(tile, jnp.int32),
            pltpu.VMEM(tile, jnp.int32),
            pltpu.VMEM((depth,) + tile, f32),
            pltpu.VMEM((STEPS,) + tile, f32),
            pltpu.VMEM((slab + depth + 2,) + tile, f32),
            pltpu.VMEM((slab + depth,) + tile, f32),
            packets, packets, packets, packets,
            pltpu.VMEM((2, depth) + tile, f32),
            dma((chunks,)), dma((7,)),
            dma((2, chunks)), dma((2, chunks)), dma((2, chunks)),
            dma((2, chunks)), dma((2, chunks)), dma((2, chunks)),
            dma, dma, dma,
            pltpu.SemaphoreType.REGULAR, pltpu.SemaphoreType.REGULAR,
        ],
        compiler_params=pltpu.CompilerParams(collective_id=0, has_side_effects=True),
        name="march",
    )(*args)
    return pl.pallas_call(
        put,
        out_shape=tuple(jax.ShapeDtypeStruct(shape, f32) for shape in shapes),
        in_specs=[pl.BlockSpec(memory_space=pltpu.VMEM)] * 2,
        out_specs=[pl.BlockSpec(memory_space=pl.ANY)] * 2,
        scratch_shapes=[dma((2,))],
        name="put",
    )(*(pltpu.with_memory_space_constraint(x, pltpu.VMEM) for x in held))


def solution(mesh):
    in_specs = (
        P(None, ("shots", "gx"), "gy"),
        P(None, ("shots", "gx"), "gy"),
        P(None, "gx", "gy"),
        P("shots"),
        P(("shots", "gx"), "gy"),
        P(("shots", "gx"), "gy"),
        P(("shots", "gx"), "gy"),
        P(None, ("shots", "gx"), "gy"),
    )
    out_specs = (P(None, ("shots", "gx"), "gy"), P("gx", "shots", "gy"))
    return jax.shard_map(
        functools.partial(shards, mesh.shape["gx"]),
        mesh=mesh, in_specs=in_specs, out_specs=out_specs, check_vma=False,
    )
```

```python
import functools

import jax
import jax.numpy as jnp
from jax import lax
from jax.experimental import pallas as pl
from jax.experimental.pallas import tpu as pltpu
from jax.sharding import PartitionSpec as P

STEPS = 8
CENTER = -205.0 / 72.0
COEFS = (1.6, -0.2, 8.0 / 315.0, -1.0 / 560.0)
REACH = 4
ROWS = 32
PAIRS = ROWS // 2
GROUP = 4
EARLY = 10
HEAD = 6
MESH = pl.DeviceIdType.MESH


def kernel(
    ring,
    pressure, prior, courant, wavelet, delay, source, receiver, snapshot,
    final, image,
    field, courant_in, courant_f32, samples, delay_v, source_v, receiver_v, snapshot_v,
    amplitude, product, filtered,
    to_left, to_right, from_left, from_right, side,
    chunk_sem, load_sem, left_send, right_send, side_send, left_recv, right_recv, side_recv,
    image_send, image_recv, out_sem, token_left, token_right,
):
    depth, width, lanes = pressure.shape
    chunks = depth // ROWS
    slab = depth // ring
    me, my_y = lax.axis_index("gx"), lax.axis_index("gy")
    right, left = lax.rem(me + 1, ring), lax.rem(me + ring - 1, ring)
    has_left, has_right = me > 0, me < ring - 1

    barrier = pltpu.get_barrier_semaphore()
    for peer in ({"gx": left}, {"gx": right}, {"gy": 1 - my_y}):
        pl.semaphore_signal(barrier, inc=1, device_id=peer, device_id_type=MESH)

    def load_chunk(c):
        return pltpu.make_async_copy(
            pressure.at[pl.ds(c * ROWS, ROWS)], field.at[0, pl.ds(REACH + c * ROWS, ROWS)],
            chunk_sem.at[c],
        )

    for c in range(chunks):
        load_chunk(c).start()
    inner = pl.ds(REACH, depth)
    loads = [
        pltpu.make_async_copy(src, dst, load_sem.at[i])
        for i, (src, dst) in enumerate(
            (
                (wavelet, samples),
                (delay, delay_v),
                (source, source_v),
                (prior, field.at[1, inner]),
                (courant, courant_in),
                (receiver, receiver_v),
                (snapshot, snapshot_v),
            )
        )
    ]
    for load in loads:
        load.start()

    zero = jnp.zeros((width, lanes), jnp.float32)
    for half in range(2):
        for i in range(REACH):
            field[half, i] = zero
            field[half, depth + REACH + i] = zero
    for i in range(slab + 1):
        product[i] = zero
    product[slab + depth + 1] = zero

    @pl.when(jnp.logical_not(has_left))
    def _():
        from_left[...] = jnp.zeros_like(from_left)

    @pl.when(jnp.logical_not(has_right))
    def _():
        from_right[...] = jnp.zeros_like(from_right)

    sub = lax.broadcasted_iota(jnp.int32, (width, lanes), 0)
    lane = lax.broadcasted_iota(jnp.int32, (width, lanes), 1)
    low = sub < REACH
    facing = (lane // (lanes // 2)) == my_y

    def left_copy(slot, c):
        return pltpu.make_async_remote_copy(
            to_left.at[slot, c], from_right.at[slot, c], left_send.at[slot, c],
            right_recv.at[slot, c], device_id={"gx": left}, device_id_type=MESH,
        )

    def right_copy(slot, c):
        return pltpu.make_async_remote_copy(
            to_right.at[slot, c], from_left.at[slot, c], right_send.at[slot, c],
            left_recv.at[slot, c], device_id={"gx": right}, device_id_type=MESH,
        )

    def side_copy(slot, c):
        return pltpu.make_async_remote_copy(
            field.at[slot, pl.ds(REACH + c * ROWS, ROWS)], side.at[slot, pl.ds(c * ROWS, ROWS)],
            side_send.at[slot, c], side_recv.at[slot, c],
            device_id={"gy": 1 - my_y}, device_id_type=MESH,
        )

    def send(slot, c):
        @pl.when(has_left)
        def _():
            left_copy(slot, c).start()

        @pl.when(has_right)
        def _():
            right_copy(slot, c).start()

        side_copy(slot, c).start()

    def sent(slot, c):
        @pl.when(has_left)
        def _():
            left_copy(slot, c).wait_send()

        @pl.when(has_right)
        def _():
            right_copy(slot, c).wait_send()

        side_copy(slot, c).wait_send()

    def arrived(slot, c):
        @pl.when(has_left)
        def _():
            right_copy(slot, c).wait_recv()

        @pl.when(has_right)
        def _():
            left_copy(slot, c).wait_recv()

        side_copy(slot, c).wait_recv()

    def pack(slot, c, i, first, second):
        turned = pltpu.roll(second, REACH, 0)
        to_left[slot, c, i] = jnp.where(low, first, turned)
        to_right[slot, c, i] = jnp.where(low, turned, first)

    def tell():
        pl.semaphore_signal(token_right, inc=1, device_id={"gx": left}, device_id_type=MESH)
        pl.semaphore_signal(token_left, inc=1, device_id={"gx": right}, device_id_type=MESH)

    def hear():
        pl.semaphore_wait(token_left, 1)
        pl.semaphore_wait(token_right, 1)

    def rounds(c):
        pl.when(lax.rem(c, 2) == 0)(tell)
        pl.when(lax.rem(c, 2) == 1)(hear)

    def advanced(now, later, z, halo, amp, where_from):
        at = z + REACH
        mine = field[now, at]
        beside = jnp.where(facing, side[now, z], 0.0)
        total = (3.0 * CENTER) * mine
        for k in range(1, REACH + 1):
            near = field[now, at + k] + field[now, at - k]
            if k == REACH:
                near = near + pltpu.roll(mine + halo, k, 0)
            else:
                near = near + pltpu.roll(jnp.where(sub >= k, mine, halo), width - k, 0)
                near = near + pltpu.roll(jnp.where(sub < width - k, mine, halo), k, 0)
            near = near + pltpu.roll(jnp.where(lane >= k, mine, beside), lanes - k, 1)
            near = near + pltpu.roll(jnp.where(lane < lanes - k, mine, beside), k, 1)
            total = total + COEFS[k - 1] * near
        added = jnp.where(where_from == z, amp, 0.0)
        return 2.0 * mine - field[later, at] + courant_f32[z] * total + added

    def halos(now, c, i):
        a, b = from_left[now, c, i], from_right[now, c, i]
        return jnp.where(low, b, a), pltpu.roll(jnp.where(low, a, b), REACH, 0)

    pl.semaphore_wait(barrier, 3)
    tell()

    def open_chunk(c, _):
        load_chunk(c).wait()
        for i in range(PAIRS):
            z = c * ROWS + 2 * i + REACH
            pack(0, c, i, field[0, z], field[0, z + 1])
        send(0, c)
        return 0

    lax.fori_loop(0, chunks, open_chunk, 0)

    for load in loads:
        load.wait()
    when = delay_v[...]
    for t in range(STEPS):
        amp = jnp.zeros((width, lanes), jnp.float32)
        for pick in range(samples.shape[0]):
            amp = amp + jnp.where(when + t == pick, samples[pick], 0.0)
        amplitude[t] = amp

    def widen(c, _):
        for i in range(ROWS):
            courant_f32[c * ROWS + i] = courant_in[c * ROWS + i].astype(jnp.float32)
        return 0

    lax.fori_loop(0, chunks, widen, 0)
    hear()

    def step(t, _):
        now, later = lax.rem(t, 2), lax.rem(t + 1, 2)

        def chunk(c, _):
            rounds(c)
            arrived(now, c)

            @pl.when(t > 0)
            def _():
                sent(later, c)

            amp, where_from = amplitude[t], source_v[...]
            for first in range(0, PAIRS, GROUP):
                pairs = [
                    [
                        advanced(now, later, c * ROWS + 2 * i + j, halo, amp, where_from)
                        for j, halo in enumerate(halos(now, c, i))
                    ]
                    for i in range(first, first + GROUP)
                ]
                for i, new in enumerate(pairs, first):
                    z = c * ROWS + 2 * i
                    field[later, z + REACH] = new[0]
                    field[later, z + REACH + 1] = new[1]
                    pack(later, c, i, *new)
            send(later, c)
            return 0

        lax.fori_loop(0, chunks, chunk, 0)
        return 0

    lax.fori_loop(0, STEPS - 1, step, 0)

    now, later = (STEPS - 1) % 2, STEPS % 2

    def block(owner):
        return filtered.at[pl.ds(slab + owner * slab, slab)]

    def place(owner):
        return image.at[:, pl.ds(pl.multiple_of(owner * width, width), width), :]

    def image_copy(owner):
        return pltpu.make_async_remote_copy(
            block(owner), place(me), image_send, image_recv,
            device_id={"gx": owner}, device_id_type=MESH,
        )

    half, owners = ring // 2, ROWS // slab

    def filter_row(first, count):
        for i in range(count):
            z = slab + first + i
            filtered[z] = 2.0 * product[z + 1] - product[z] - product[z + 2]

    def early(owner):
        ahead = lax.rem(owner - me + ring, ring)
        far = jnp.minimum(ahead, ring - ahead) >= EARLY
        return far & (owner >= 0) & (owner < (chunks - 1) * owners - 1)

    def last_chunk(c, _):
        arrived(now, c)
        sent(later, c)
        amp, where_from, first_level = amplitude[STEPS - 1], source_v[...], receiver_v[...]
        for i in range(PAIRS):
            for j, halo in enumerate(halos(now, c, i)):
                z = c * ROWS + 2 * i + j
                new = advanced(now, later, z, halo, amp, where_from)
                final[z] = new
                product[slab + z + 1] = new * jnp.where(first_level <= z, snapshot_v[z], 0.0)
        filter_row(c * ROWS - slab, ROWS)
        for i in range(owners):
            owner = c * owners - 1 + i

            @pl.when(early(owner))
            def _():
                image_copy(owner).start()

        return 0

    lax.fori_loop(0, chunks, last_chunk, 0)

    filter_row(depth - slab, slab)

    def send_block(owner):
        @pl.when(jnp.logical_not(early(owner)))
        def _():
            image_copy(owner).start()

    send_block(lax.rem(me + half, ring))

    def spread(i, _):
        key = half - 1 + HEAD - i
        for k, low_owner in ((key, False), (key - HEAD, True)):
            for owner in (lax.rem(me + k + ring, ring), lax.rem(me - k + ring, ring)):
                @pl.when((k >= 1) & (k < half) & ((owner < ring // 8) == low_owner))
                def _():
                    send_block(owner)

        return 0

    lax.fori_loop(0, half - 1 + HEAD, spread, 0)
    own = pltpu.make_async_copy(block(me), place(me), out_sem)
    own.start()

    def drain(c, _):
        sent(now, c)
        return 0

    lax.fori_loop(0, chunks, drain, 0)
    own.wait()

    rest = image.at[:, pl.ds(0, (ring - 1) * width), :]
    pltpu.make_async_copy(rest, rest, image_recv).wait()
    pltpu.make_async_copy(rest, rest, image_send).wait()


def put(final_in, image_in, final, image, sems):
    copies = [
        pltpu.make_async_copy(final_in, final, sems.at[0]),
        pltpu.make_async_copy(image_in, image, sems.at[1]),
    ]
    for copy in copies:
        copy.start()
    for copy in copies:
        copy.wait()


def shards(ring, *args):
    pressure = args[0]
    depth, width, lanes = pressure.shape
    chunks, slab = depth // ROWS, depth // ring
    tile = (width, lanes)
    f32 = jnp.float32
    packets = pltpu.VMEM((2, chunks, PAIRS) + tile, f32)
    dma = pltpu.SemaphoreType.DMA
    shapes = ((depth,) + tile, (slab, ring * width, lanes))
    held = pl.pallas_call(
        functools.partial(kernel, ring),
        out_shape=tuple(pltpu.VMEM(shape, f32) for shape in shapes),
        in_specs=[pl.BlockSpec(memory_space=pl.ANY)] * 8,
        out_specs=[pl.BlockSpec(memory_space=pltpu.VMEM)] * 2,
        scratch_shapes=[
            pltpu.VMEM((2, depth + 2 * REACH) + tile, f32),
            pltpu.VMEM((depth,) + tile, jnp.bfloat16),
            pltpu.VMEM((depth,) + tile, f32),
            pltpu.SMEM(args[3].shape, f32),
            pltpu.VMEM(tile, jnp.int32),
            pltpu.VMEM(tile, jnp.int32),
            pltpu.VMEM(tile, jnp.int32),
            pltpu.VMEM((depth,) + tile, f32),
            pltpu.VMEM((STEPS,) + tile, f32),
            pltpu.VMEM((slab + depth + 2,) + tile, f32),
            pltpu.VMEM((slab + depth,) + tile, f32),
            packets, packets, packets, packets,
            pltpu.VMEM((2, depth) + tile, f32),
            dma((chunks,)), dma((7,)),
            dma((2, chunks)), dma((2, chunks)), dma((2, chunks)),
            dma((2, chunks)), dma((2, chunks)), dma((2, chunks)),
            dma, dma, dma,
            pltpu.SemaphoreType.REGULAR, pltpu.SemaphoreType.REGULAR,
        ],
        compiler_params=pltpu.CompilerParams(collective_id=0, has_side_effects=True),
        name="march",
    )(*args)
    return pl.pallas_call(
        put,
        out_shape=tuple(jax.ShapeDtypeStruct(shape, f32) for shape in shapes),
        in_specs=[pl.BlockSpec(memory_space=pltpu.VMEM)] * 2,
        out_specs=[pl.BlockSpec(memory_space=pl.ANY)] * 2,
        scratch_shapes=[dma((2,))],
        name="put",
    )(*(pltpu.with_memory_space_constraint(x, pltpu.VMEM) for x in held))


def solution(mesh):
    in_specs = (
        P(None, ("shots", "gx"), "gy"),
        P(None, ("shots", "gx"), "gy"),
        P(None, "gx", "gy"),
        P("shots"),
        P(("shots", "gx"), "gy"),
        P(("shots", "gx"), "gy"),
        P(("shots", "gx"), "gy"),
        P(None, ("shots", "gx"), "gy"),
    )
    out_specs = (P(None, ("shots", "gx"), "gy"), P("gx", "shots", "gy"))
    return jax.shard_map(
        functools.partial(shards, mesh.shape["gx"]),
        mesh=mesh, in_specs=in_specs, out_specs=out_specs, check_vma=False,
    )
```

```python
import functools

import jax
import jax.numpy as jnp
from jax import lax
from jax.experimental import pallas as pl
from jax.experimental.pallas import tpu as pltpu
from jax.sharding import PartitionSpec as P

STEPS = 8
CENTER = -205.0 / 72.0
COEFS = (1.6, -0.2, 8.0 / 315.0, -1.0 / 560.0)
REACH = 4
ROWS = 32
PAIRS = ROWS // 2
GROUP = 4
EARLY = 12
HEAD = 6
MESH = pl.DeviceIdType.MESH


def kernel(
    ring,
    pressure, prior, courant, wavelet, delay, source, receiver, snapshot,
    final, image,
    field, courant_in, courant_f32, samples, delay_v, source_v, receiver_v, snapshot_v,
    amplitude, product, filtered,
    to_left, to_right, from_left, from_right, side,
    chunk_sem, load_sem, left_send, right_send, side_send, left_recv, right_recv, side_recv,
    image_send, image_recv, out_sem, token_left, token_right,
):
    depth, width, lanes = pressure.shape
    chunks = depth // ROWS
    slab = depth // ring
    me, my_y = lax.axis_index("gx"), lax.axis_index("gy")
    right, left = lax.rem(me + 1, ring), lax.rem(me + ring - 1, ring)
    has_left, has_right = me > 0, me < ring - 1

    barrier = pltpu.get_barrier_semaphore()
    for peer in ({"gx": left}, {"gx": right}, {"gy": 1 - my_y}):
        pl.semaphore_signal(barrier, inc=1, device_id=peer, device_id_type=MESH)

    def load_chunk(c):
        return pltpu.make_async_copy(
            pressure.at[pl.ds(c * ROWS, ROWS)], field.at[0, pl.ds(REACH + c * ROWS, ROWS)],
            chunk_sem.at[c],
        )

    for c in range(chunks):
        load_chunk(c).start()
    inner = pl.ds(REACH, depth)
    loads = [
        pltpu.make_async_copy(src, dst, load_sem.at[i])
        for i, (src, dst) in enumerate(
            (
                (wavelet, samples),
                (delay, delay_v),
                (source, source_v),
                (prior, field.at[1, inner]),
                (courant, courant_in),
                (receiver, receiver_v),
                (snapshot, snapshot_v),
            )
        )
    ]
    for load in loads:
        load.start()

    zero = jnp.zeros((width, lanes), jnp.float32)
    for half in range(2):
        for i in range(REACH):
            field[half, i] = zero
            field[half, depth + REACH + i] = zero
    for i in range(slab + 1):
        product[i] = zero
    product[slab + depth + 1] = zero

    @pl.when(jnp.logical_not(has_left))
    def _():
        from_left[...] = jnp.zeros_like(from_left)

    @pl.when(jnp.logical_not(has_right))
    def _():
        from_right[...] = jnp.zeros_like(from_right)

    sub = lax.broadcasted_iota(jnp.int32, (width, lanes), 0)
    lane = lax.broadcasted_iota(jnp.int32, (width, lanes), 1)
    low = sub < REACH
    facing = (lane // (lanes // 2)) == my_y

    def left_copy(slot, c):
        return pltpu.make_async_remote_copy(
            to_left.at[slot, c], from_right.at[slot, c], left_send.at[slot, c],
            right_recv.at[slot, c], device_id={"gx": left}, device_id_type=MESH,
        )

    def right_copy(slot, c):
        return pltpu.make_async_remote_copy(
            to_right.at[slot, c], from_left.at[slot, c], right_send.at[slot, c],
            left_recv.at[slot, c], device_id={"gx": right}, device_id_type=MESH,
        )

    def side_copy(slot, c):
        return pltpu.make_async_remote_copy(
            field.at[slot, pl.ds(REACH + c * ROWS, ROWS)], side.at[slot, pl.ds(c * ROWS, ROWS)],
            side_send.at[slot, c], side_recv.at[slot, c],
            device_id={"gy": 1 - my_y}, device_id_type=MESH,
        )

    def send(slot, c):
        @pl.when(has_left)
        def _():
            left_copy(slot, c).start()

        @pl.when(has_right)
        def _():
            right_copy(slot, c).start()

        side_copy(slot, c).start()

    def sent(slot, c):
        @pl.when(has_left)
        def _():
            left_copy(slot, c).wait_send()

        @pl.when(has_right)
        def _():
            right_copy(slot, c).wait_send()

        side_copy(slot, c).wait_send()

    def arrived(slot, c):
        @pl.when(has_left)
        def _():
            right_copy(slot, c).wait_recv()

        @pl.when(has_right)
        def _():
            left_copy(slot, c).wait_recv()

        side_copy(slot, c).wait_recv()

    def pack(slot, c, i, first, second):
        turned = pltpu.roll(second, REACH, 0)
        to_left[slot, c, i] = jnp.where(low, first, turned)
        to_right[slot, c, i] = jnp.where(low, turned, first)

    def tell():
        pl.semaphore_signal(token_right, inc=1, device_id={"gx": left}, device_id_type=MESH)
        pl.semaphore_signal(token_left, inc=1, device_id={"gx": right}, device_id_type=MESH)

    def hear():
        pl.semaphore_wait(token_left, 1)
        pl.semaphore_wait(token_right, 1)

    def rounds(c):
        pl.when(lax.rem(c, 2) == 0)(tell)
        pl.when(lax.rem(c, 2) == 1)(hear)

    def advanced(now, later, z, halo, amp, where_from):
        at = z + REACH
        mine = field[now, at]
        beside = jnp.where(facing, side[now, z], 0.0)
        total = (3.0 * CENTER) * mine
        for k in range(1, REACH + 1):
            near = field[now, at + k] + field[now, at - k]
            if k == REACH:
                near = near + pltpu.roll(mine + halo, k, 0)
            else:
                near = near + pltpu.roll(jnp.where(sub >= k, mine, halo), width - k, 0)
                near = near + pltpu.roll(jnp.where(sub < width - k, mine, halo), k, 0)
            near = near + pltpu.roll(jnp.where(lane >= k, mine, beside), lanes - k, 1)
            near = near + pltpu.roll(jnp.where(lane < lanes - k, mine, beside), k, 1)
            total = total + COEFS[k - 1] * near
        added = jnp.where(where_from == z, amp, 0.0)
        return 2.0 * mine - field[later, at] + courant_f32[z] * total + added

    def halos(now, c, i):
        a, b = from_left[now, c, i], from_right[now, c, i]
        return jnp.where(low, b, a), pltpu.roll(jnp.where(low, a, b), REACH, 0)

    def open_chunk(c, _):
        load_chunk(c).wait()
        for i in range(PAIRS):
            z = c * ROWS + 2 * i + REACH
            pack(0, c, i, field[0, z], field[0, z + 1])
        return 0

    lax.fori_loop(0, chunks, open_chunk, 0)
    pl.semaphore_wait(barrier, 3)

    def open_send(c, _):
        send(0, c)
        return 0

    lax.fori_loop(0, chunks, open_send, 0)
    tell()

    for load in loads:
        load.wait()
    when = delay_v[...]
    for t in range(STEPS):
        amp = jnp.zeros((width, lanes), jnp.float32)
        for pick in range(samples.shape[0]):
            amp = amp + jnp.where(when + t == pick, samples[pick], 0.0)
        amplitude[t] = amp

    def widen(c, _):
        for i in range(ROWS):
            courant_f32[c * ROWS + i] = courant_in[c * ROWS + i].astype(jnp.float32)
        return 0

    lax.fori_loop(0, chunks, widen, 0)
    hear()

    def step(t, _):
        now, later = lax.rem(t, 2), lax.rem(t + 1, 2)

        def chunk(c, _):
            rounds(c)
            arrived(now, c)

            @pl.when(t > 0)
            def _():
                sent(later, c)

            amp, where_from = amplitude[t], source_v[...]
            for first in range(0, PAIRS, GROUP):
                pairs = [
                    [
                        advanced(now, later, c * ROWS + 2 * i + j, halo, amp, where_from)
                        for j, halo in enumerate(halos(now, c, i))
                    ]
                    for i in range(first, first + GROUP)
                ]
                for i, new in enumerate(pairs, first):
                    z = c * ROWS + 2 * i
                    field[later, z + REACH] = new[0]
                    field[later, z + REACH + 1] = new[1]
                    pack(later, c, i, *new)
            send(later, c)
            return 0

        lax.fori_loop(0, chunks, chunk, 0)
        return 0

    lax.fori_loop(0, STEPS - 1, step, 0)

    now, later = (STEPS - 1) % 2, STEPS % 2

    def block(owner):
        return filtered.at[pl.ds(slab + owner * slab, slab)]

    def place(owner):
        return image.at[:, pl.ds(pl.multiple_of(owner * width, width), width), :]

    def image_copy(owner):
        return pltpu.make_async_remote_copy(
            block(owner), place(me), image_send, image_recv,
            device_id={"gx": owner}, device_id_type=MESH,
        )

    half, owners = ring // 2, ROWS // slab

    def filter_row(first, count):
        for i in range(count):
            z = slab + first + i
            filtered[z] = 2.0 * product[z + 1] - product[z] - product[z + 2]

    def early(owner):
        ahead = lax.rem(owner - me + ring, ring)
        far = jnp.minimum(ahead, ring - ahead) >= EARLY
        return far & (owner >= 0) & (owner < (chunks - 1) * owners - 1)

    def last_chunk(c, _):
        arrived(now, c)
        sent(later, c)
        amp, where_from, first_level = amplitude[STEPS - 1], source_v[...], receiver_v[...]
        for i in range(PAIRS):
            for j, halo in enumerate(halos(now, c, i)):
                z = c * ROWS + 2 * i + j
                new = advanced(now, later, z, halo, amp, where_from)
                final[z] = new
                product[slab + z + 1] = new * jnp.where(first_level <= z, snapshot_v[z], 0.0)
        filter_row(c * ROWS - slab, ROWS)
        for i in range(owners):
            owner = c * owners - 1 + i

            @pl.when(early(owner))
            def _():
                image_copy(owner).start()

        return 0

    lax.fori_loop(0, chunks, last_chunk, 0)

    filter_row(depth - slab, slab)

    def send_block(owner):
        @pl.when(jnp.logical_not(early(owner)))
        def _():
            image_copy(owner).start()

    send_block(lax.rem(me + half, ring))

    def spread(i, _):
        key = half - 1 + HEAD - i
        for k, low_owner in ((key, False), (key - HEAD, True)):
            for owner in (lax.rem(me + k + ring, ring), lax.rem(me - k + ring, ring)):
                @pl.when((k >= 1) & (k < half) & ((owner < ring // 8) == low_owner))
                def _():
                    send_block(owner)

        return 0

    lax.fori_loop(0, half - 1 + HEAD, spread, 0)
    own = pltpu.make_async_copy(block(me), place(me), out_sem)
    own.start()

    def drain(c, _):
        sent(now, c)
        return 0

    lax.fori_loop(0, chunks, drain, 0)
    own.wait()

    rest = image.at[:, pl.ds(0, (ring - 1) * width), :]
    pltpu.make_async_copy(rest, rest, image_recv).wait()
    pltpu.make_async_copy(rest, rest, image_send).wait()


def put(final_in, image_in, final, image, sems):
    copies = [
        pltpu.make_async_copy(final_in, final, sems.at[0]),
        pltpu.make_async_copy(image_in, image, sems.at[1]),
    ]
    for copy in copies:
        copy.start()
    for copy in copies:
        copy.wait()


def shards(ring, *args):
    pressure = args[0]
    depth, width, lanes = pressure.shape
    chunks, slab = depth // ROWS, depth // ring
    tile = (width, lanes)
    f32 = jnp.float32
    packets = pltpu.VMEM((2, chunks, PAIRS) + tile, f32)
    dma = pltpu.SemaphoreType.DMA
    shapes = ((depth,) + tile, (slab, ring * width, lanes))
    held = pl.pallas_call(
        functools.partial(kernel, ring),
        out_shape=tuple(pltpu.VMEM(shape, f32) for shape in shapes),
        in_specs=[pl.BlockSpec(memory_space=pl.ANY)] * 8,
        out_specs=[pl.BlockSpec(memory_space=pltpu.VMEM)] * 2,
        scratch_shapes=[
            pltpu.VMEM((2, depth + 2 * REACH) + tile, f32),
            pltpu.VMEM((depth,) + tile, jnp.bfloat16),
            pltpu.VMEM((depth,) + tile, f32),
            pltpu.SMEM(args[3].shape, f32),
            pltpu.VMEM(tile, jnp.int32),
            pltpu.VMEM(tile, jnp.int32),
            pltpu.VMEM(tile, jnp.int32),
            pltpu.VMEM((depth,) + tile, f32),
            pltpu.VMEM((STEPS,) + tile, f32),
            pltpu.VMEM((slab + depth + 2,) + tile, f32),
            pltpu.VMEM((slab + depth,) + tile, f32),
            packets, packets, packets, packets,
            pltpu.VMEM((2, depth) + tile, f32),
            dma((chunks,)), dma((7,)),
            dma((2, chunks)), dma((2, chunks)), dma((2, chunks)),
            dma((2, chunks)), dma((2, chunks)), dma((2, chunks)),
            dma, dma, dma,
            pltpu.SemaphoreType.REGULAR, pltpu.SemaphoreType.REGULAR,
        ],
        compiler_params=pltpu.CompilerParams(collective_id=0, has_side_effects=True),
        name="march",
    )(*args)
    return pl.pallas_call(
        put,
        out_shape=tuple(jax.ShapeDtypeStruct(shape, f32) for shape in shapes),
        in_specs=[pl.BlockSpec(memory_space=pltpu.VMEM)] * 2,
        out_specs=[pl.BlockSpec(memory_space=pl.ANY)] * 2,
        scratch_shapes=[dma((2,))],
        name="put",
    )(*(pltpu.with_memory_space_constraint(x, pltpu.VMEM) for x in held))


def solution(mesh):
    in_specs = (
        P(None, ("shots", "gx"), "gy"),
        P(None, ("shots", "gx"), "gy"),
        P(None, "gx", "gy"),
        P("shots"),
        P(("shots", "gx"), "gy"),
        P(("shots", "gx"), "gy"),
        P(("shots", "gx"), "gy"),
        P(None, ("shots", "gx"), "gy"),
    )
    out_specs = (P(None, ("shots", "gx"), "gy"), P("gx", "shots", "gy"))
    return jax.shard_map(
        functools.partial(shards, mesh.shape["gx"]),
        mesh=mesh, in_specs=in_specs, out_specs=out_specs, check_vma=False,
    )
```

```python
import functools

import jax
import jax.numpy as jnp
from jax import lax
from jax.experimental import pallas as pl
from jax.experimental.pallas import tpu as pltpu
from jax.sharding import PartitionSpec as P

STEPS = 8
CENTER = -205.0 / 72.0
COEFS = (1.6, -0.2, 8.0 / 315.0, -1.0 / 560.0)
REACH = 4
ROWS = 32
PAIRS = ROWS // 2
GROUP = 4
EARLY = 12
HEAD = 6
MESH = pl.DeviceIdType.MESH


def kernel(
    ring,
    pressure, prior, courant, wavelet, delay, source, receiver, snapshot,
    final, image,
    field, courant_in, courant_f32, samples, delay_v, source_v, receiver_v, snapshot_v,
    amplitude, product, filtered,
    to_left, to_right, from_left, from_right, side,
    chunk_sem, load_sem, left_send, right_send, side_send, left_recv, right_recv, side_recv,
    image_send, image_recv, out_sem, token_left, token_right,
):
    depth, width, lanes = pressure.shape
    chunks = depth // ROWS
    slab = depth // ring
    me, my_y = lax.axis_index("gx"), lax.axis_index("gy")
    right, left = lax.rem(me + 1, ring), lax.rem(me + ring - 1, ring)
    has_left, has_right = me > 0, me < ring - 1

    barrier = pltpu.get_barrier_semaphore()
    for peer in ({"gx": left}, {"gx": right}, {"gy": 1 - my_y}):
        pl.semaphore_signal(barrier, inc=1, device_id=peer, device_id_type=MESH)

    def load_chunk(c):
        return pltpu.make_async_copy(
            pressure.at[pl.ds(c * ROWS, ROWS)], field.at[0, pl.ds(REACH + c * ROWS, ROWS)],
            chunk_sem.at[c],
        )

    for c in range(chunks):
        load_chunk(c).start()
    inner = pl.ds(REACH, depth)
    loads = [
        pltpu.make_async_copy(src, dst, load_sem.at[i])
        for i, (src, dst) in enumerate(
            (
                (wavelet, samples),
                (delay, delay_v),
                (source, source_v),
                (prior, field.at[1, inner]),
                (courant, courant_in),
                (receiver, receiver_v),
                (snapshot, snapshot_v),
            )
        )
    ]
    for load in loads:
        load.start()

    zero = jnp.zeros((width, lanes), jnp.float32)
    for half in range(2):
        for i in range(REACH):
            field[half, i] = zero
            field[half, depth + REACH + i] = zero
    for i in range(slab + 1):
        product[i] = zero
    product[slab + depth + 1] = zero

    @pl.when(jnp.logical_not(has_left))
    def _():
        from_left[...] = jnp.zeros_like(from_left)

    @pl.when(jnp.logical_not(has_right))
    def _():
        from_right[...] = jnp.zeros_like(from_right)

    sub = lax.broadcasted_iota(jnp.int32, (width, lanes), 0)
    lane = lax.broadcasted_iota(jnp.int32, (width, lanes), 1)
    low = sub < REACH
    facing = (lane // (lanes // 2)) == my_y

    def left_copy(slot, c):
        return pltpu.make_async_remote_copy(
            to_left.at[slot, c], from_right.at[slot, c], left_send.at[slot, c],
            right_recv.at[slot, c], device_id={"gx": left}, device_id_type=MESH,
        )

    def right_copy(slot, c):
        return pltpu.make_async_remote_copy(
            to_right.at[slot, c], from_left.at[slot, c], right_send.at[slot, c],
            left_recv.at[slot, c], device_id={"gx": right}, device_id_type=MESH,
        )

    def side_copy(slot, c):
        return pltpu.make_async_remote_copy(
            field.at[slot, pl.ds(REACH + c * ROWS, ROWS)], side.at[slot, pl.ds(c * ROWS, ROWS)],
            side_send.at[slot, c], side_recv.at[slot, c],
            device_id={"gy": 1 - my_y}, device_id_type=MESH,
        )

    def send(slot, c):
        @pl.when(has_left)
        def _():
            left_copy(slot, c).start()

        @pl.when(has_right)
        def _():
            right_copy(slot, c).start()

        side_copy(slot, c).start()

    def sent(slot, c):
        @pl.when(has_left)
        def _():
            left_copy(slot, c).wait_send()

        @pl.when(has_right)
        def _():
            right_copy(slot, c).wait_send()

        side_copy(slot, c).wait_send()

    def arrived(slot, c):
        @pl.when(has_left)
        def _():
            right_copy(slot, c).wait_recv()

        @pl.when(has_right)
        def _():
            left_copy(slot, c).wait_recv()

        side_copy(slot, c).wait_recv()

    def pack(slot, c, i, first, second):
        turned = pltpu.roll(second, REACH, 0)
        to_left[slot, c, i] = jnp.where(low, first, turned)
        to_right[slot, c, i] = jnp.where(low, turned, first)

    def tell():
        pl.semaphore_signal(token_right, inc=1, device_id={"gx": left}, device_id_type=MESH)
        pl.semaphore_signal(token_left, inc=1, device_id={"gx": right}, device_id_type=MESH)

    def hear():
        pl.semaphore_wait(token_left, 1)
        pl.semaphore_wait(token_right, 1)

    def rounds(c):
        pl.when(lax.rem(c, 2) == 0)(tell)
        pl.when(lax.rem(c, 2) == 1)(hear)

    def advanced(now, later, z, halo, amp, where_from):
        at = z + REACH
        mine = field[now, at]
        beside = jnp.where(facing, side[now, z], 0.0)
        total = (3.0 * CENTER) * mine
        for k in range(1, REACH + 1):
            near = field[now, at + k] + field[now, at - k]
            if k == REACH:
                near = near + pltpu.roll(mine + halo, k, 0)
            else:
                near = near + pltpu.roll(jnp.where(sub >= k, mine, halo), width - k, 0)
                near = near + pltpu.roll(jnp.where(sub < width - k, mine, halo), k, 0)
            near = near + pltpu.roll(jnp.where(lane >= k, mine, beside), lanes - k, 1)
            near = near + pltpu.roll(jnp.where(lane < lanes - k, mine, beside), k, 1)
            total = total + COEFS[k - 1] * near
        added = jnp.where(where_from == z, amp, 0.0)
        return 2.0 * mine - field[later, at] + courant_f32[z] * total + added

    def halos(now, c, i):
        a, b = from_left[now, c, i], from_right[now, c, i]
        return jnp.where(low, b, a), pltpu.roll(jnp.where(low, a, b), REACH, 0)

    def open_chunk(c, _):
        load_chunk(c).wait()
        for i in range(PAIRS):
            z = c * ROWS + 2 * i + REACH
            pack(0, c, i, field[0, z], field[0, z + 1])
        return 0

    lax.fori_loop(0, chunks, open_chunk, 0)
    pl.semaphore_wait(barrier, 3)

    def open_send(c, _):
        send(0, c)
        return 0

    lax.fori_loop(0, chunks, open_send, 0)
    tell()

    for load in loads:
        load.wait()
    when = delay_v[...]
    for t in range(STEPS):
        amp = jnp.zeros((width, lanes), jnp.float32)
        for pick in range(samples.shape[0]):
            amp = amp + jnp.where(when + t == pick, samples[pick], 0.0)
        amplitude[t] = amp

    def widen(c, _):
        for i in range(ROWS):
            courant_f32[c * ROWS + i] = courant_in[c * ROWS + i].astype(jnp.float32)
        return 0

    lax.fori_loop(0, chunks, widen, 0)
    hear()

    def step(t, _):
        now, later = lax.rem(t, 2), lax.rem(t + 1, 2)

        def chunk(c, _):
            rounds(c)
            arrived(now, c)

            @pl.when(t > 0)
            def _():
                sent(later, c)

            amp, where_from = amplitude[t], source_v[...]
            for first in range(0, PAIRS, GROUP):
                pairs = [
                    [
                        advanced(now, later, c * ROWS + 2 * i + j, halo, amp, where_from)
                        for j, halo in enumerate(halos(now, c, i))
                    ]
                    for i in range(first, first + GROUP)
                ]
                for i, new in enumerate(pairs, first):
                    z = c * ROWS + 2 * i
                    field[later, z + REACH] = new[0]
                    field[later, z + REACH + 1] = new[1]
                    pack(later, c, i, *new)
            send(later, c)
            return 0

        lax.fori_loop(0, chunks, chunk, 0)
        return 0

    lax.fori_loop(0, STEPS - 1, step, 0)

    now, later = (STEPS - 1) % 2, STEPS % 2

    def block(owner):
        return filtered.at[pl.ds(slab + owner * slab, slab)]

    def place(owner):
        return image.at[:, pl.ds(pl.multiple_of(owner * width, width), width), :]

    def image_copy(owner):
        return pltpu.make_async_remote_copy(
            block(owner), place(me), image_send, image_recv,
            device_id={"gx": owner}, device_id_type=MESH,
        )

    half, owners = ring // 2, ROWS // slab

    def filter_row(first, count):
        for i in range(count):
            z = slab + first + i
            filtered[z] = 2.0 * product[z + 1] - product[z] - product[z + 2]

    def early(owner):
        ahead = lax.rem(owner - me + ring, ring)
        far = jnp.minimum(ahead, ring - ahead) >= EARLY
        return far & (owner >= 0) & (owner < (chunks - 1) * owners - 1)

    def last_chunk(c, _):
        arrived(now, c)
        sent(later, c)
        amp, where_from, first_level = amplitude[STEPS - 1], source_v[...], receiver_v[...]
        for i in range(PAIRS):
            for j, halo in enumerate(halos(now, c, i)):
                z = c * ROWS + 2 * i + j
                new = advanced(now, later, z, halo, amp, where_from)
                final[z] = new
                product[slab + z + 1] = new * jnp.where(first_level <= z, snapshot_v[z], 0.0)
        filter_row(c * ROWS - slab, ROWS)
        for i in range(owners):
            owner = c * owners - 1 + i

            @pl.when(early(owner))
            def _():
                image_copy(owner).start()

        return 0

    lax.fori_loop(0, chunks, last_chunk, 0)

    filter_row(depth - slab, slab)

    def send_block(owner):
        @pl.when(jnp.logical_not(early(owner)))
        def _():
            image_copy(owner).start()

    send_block(lax.rem(me + half, ring))

    def spread(i, _):
        key = half - 1 + HEAD - i
        for k, low_owner in ((key, False), (key - HEAD, True)):
            for owner in (lax.rem(me + k + ring, ring), lax.rem(me - k + ring, ring)):
                @pl.when((k >= 1) & (k < half) & ((owner < ring // 16) == low_owner))
                def _():
                    send_block(owner)

        return 0

    lax.fori_loop(0, half - 1 + HEAD, spread, 0)
    own = pltpu.make_async_copy(block(me), place(me), out_sem)
    own.start()

    def drain(c, _):
        sent(now, c)
        return 0

    lax.fori_loop(0, chunks, drain, 0)
    own.wait()

    rest = image.at[:, pl.ds(0, (ring - 1) * width), :]
    pltpu.make_async_copy(rest, rest, image_recv).wait()
    pltpu.make_async_copy(rest, rest, image_send).wait()


def put(final_in, image_in, final, image, sems):
    copies = [
        pltpu.make_async_copy(final_in, final, sems.at[0]),
        pltpu.make_async_copy(image_in, image, sems.at[1]),
    ]
    for copy in copies:
        copy.start()
    for copy in copies:
        copy.wait()


def shards(ring, *args):
    pressure = args[0]
    depth, width, lanes = pressure.shape
    chunks, slab = depth // ROWS, depth // ring
    tile = (width, lanes)
    f32 = jnp.float32
    packets = pltpu.VMEM((2, chunks, PAIRS) + tile, f32)
    dma = pltpu.SemaphoreType.DMA
    shapes = ((depth,) + tile, (slab, ring * width, lanes))
    held = pl.pallas_call(
        functools.partial(kernel, ring),
        out_shape=tuple(pltpu.VMEM(shape, f32) for shape in shapes),
        in_specs=[pl.BlockSpec(memory_space=pl.ANY)] * 8,
        out_specs=[pl.BlockSpec(memory_space=pltpu.VMEM)] * 2,
        scratch_shapes=[
            pltpu.VMEM((2, depth + 2 * REACH) + tile, f32),
            pltpu.VMEM((depth,) + tile, jnp.bfloat16),
            pltpu.VMEM((depth,) + tile, f32),
            pltpu.SMEM(args[3].shape, f32),
            pltpu.VMEM(tile, jnp.int32),
            pltpu.VMEM(tile, jnp.int32),
            pltpu.VMEM(tile, jnp.int32),
            pltpu.VMEM((depth,) + tile, f32),
            pltpu.VMEM((STEPS,) + tile, f32),
            pltpu.VMEM((slab + depth + 2,) + tile, f32),
            pltpu.VMEM((slab + depth,) + tile, f32),
            packets, packets, packets, packets,
            pltpu.VMEM((2, depth) + tile, f32),
            dma((chunks,)), dma((7,)),
            dma((2, chunks)), dma((2, chunks)), dma((2, chunks)),
            dma((2, chunks)), dma((2, chunks)), dma((2, chunks)),
            dma, dma, dma,
            pltpu.SemaphoreType.REGULAR, pltpu.SemaphoreType.REGULAR,
        ],
        compiler_params=pltpu.CompilerParams(collective_id=0, has_side_effects=True),
        name="march",
    )(*args)
    return pl.pallas_call(
        put,
        out_shape=tuple(jax.ShapeDtypeStruct(shape, f32) for shape in shapes),
        in_specs=[pl.BlockSpec(memory_space=pltpu.VMEM)] * 2,
        out_specs=[pl.BlockSpec(memory_space=pl.ANY)] * 2,
        scratch_shapes=[dma((2,))],
        name="put",
    )(*(pltpu.with_memory_space_constraint(x, pltpu.VMEM) for x in held))


def solution(mesh):
    in_specs = (
        P(None, ("shots", "gx"), "gy"),
        P(None, ("shots", "gx"), "gy"),
        P(None, "gx", "gy"),
        P("shots"),
        P(("shots", "gx"), "gy"),
        P(("shots", "gx"), "gy"),
        P(("shots", "gx"), "gy"),
        P(None, ("shots", "gx"), "gy"),
    )
    out_specs = (P(None, ("shots", "gx"), "gy"), P("gx", "shots", "gy"))
    return jax.shard_map(
        functools.partial(shards, mesh.shape["gx"]),
        mesh=mesh, in_specs=in_specs, out_specs=out_specs, check_vma=False,
    )
```
